128 devices in a mesh: section: 16 (over x_lo, y, core), tensor: 4 (over z), dp: 2 (over x_hi).
Axes of the slice: x: 4 (x_hi: 2, x_lo: 2; x = x_hi * 2 + x_lo), y: 4, z: 4, core: 2. Of those that a mesh axis runs over, the one named last changes fastest.
Arguments:
- section_up: bfloat16 [16, 4096, 7168], P('section', 'dp', 'tensor'), may hold values from -0.09375 to 0.09375
- section_down: bfloat16 [16, 4096, 7168], P('section', 'dp', 'tensor'), may hold values from -0.0625 to 0.0625
- backup_up: bfloat16 [2, 16, 4, 32, 7168], P('dp', 'section', 'tensor'), may hold values from -0.09375 to 0.09375
- backup_down: bfloat16 [2, 16, 4, 32, 7168], P('dp', 'section', 'tensor'), may hold values from -0.0625 to 0.0625
- norm_gain: float32 [16, 4096], P('section'), may hold values from 0.25 to 1.75
- micro_batches: bfloat16 [16, 64, 4096], P(None, 'dp', 'tensor'), may hold values from -24 to 24
- failed_section: int32 [1], replicated, may hold values from 0 to 1048575
- live_batches: int32 [1], replicated, may hold values from 0 to 589823
Outputs:
- finals: bfloat16 [16, 64, 4096], P('section', 'dp', 'tensor')
The draws below stay inside these ranges and needn't reach their ends.
Inputs may be any that keep to these rules, and one draw needn't show every extreme that they name: failed_section modulo the number of sections names the failed section. micro-batches 0 to 16 // 2 + (live_batches modulo (16 - 16 // 2 + 1)) - 1 run.
All inputs are finite; a program needn't handle non-finite values.
Results may differ from the reference program's by a relative error of at most 0.03.
Values may be sent and summed in bfloat16 or wider, within the bound.
A program may use at most 192 MiB of HBM per device.

```python
import math
import jax
import jax.numpy as jnp
from jax import lax

D = 4096
FF = 7168
MB = 16
TOKENS_MB = 64
ROWS_PIECE = 32
N_SECTION = 16
N_TENSOR = 4
N_DP = 2


def draw_micro_batches(key, part):
    first, second, third = jax.random.split(key, 3)
    shape = (MB, TOKENS_MB, D)
    row_scale = jnp.exp(jax.random.uniform(second, (MB, TOKENS_MB, 1), jnp.float32, math.log(0.3), math.log(3.0)))
    column_scale = jnp.exp(jax.random.uniform(third, (1, 1, D), jnp.float32, math.log(0.3), math.log(3.0)))
    values = jax.random.normal(first, shape, jnp.float32) * row_scale * column_scale
    return jnp.clip(values, -24.0, 24.0).astype(jnp.bfloat16)


def shard_levels(rng, extent, pieces, smallest, top_value):
    factor_of = 1.0
    for dim, shards_of in pieces:
        draws = jax.random.uniform(jax.random.fold_in(jax.random.fold_in(rng, 6), dim), (shards_of,), jnp.float32, smallest / len(pieces), top_value / len(pieces))
        factor_of = factor_of * jnp.repeat(jnp.exp(draws), extent[dim] // shards_of).reshape((-1,) + (1,) * (len(extent) - 1 - dim))
    return factor_of


def gaussian(key, shape, deviation, limit, shards=(), kind=jnp.bfloat16):
    entries = jax.random.normal(key, shape, jnp.float32) * deviation
    if len(shards) > 0:
        entries = shard_levels(key, shape, shards, -0.22, 0.18) * entries
    return jnp.clip(entries, min=-limit, max=limit).astype(kind)


def setup_inputs(seed: int = 0) -> dict:
    key_of = jax.random.split(jax.random.key(seed), 9)
    section_up = gaussian(key_of[0], (N_SECTION, D, FF), D ** -0.5, 0.09375, ((0, 16), (1, 2), (2, 4)))
    section_down = gaussian(key_of[1], (N_SECTION, D, FF), FF ** -0.5, 0.0625, ((0, 16), (1, 2), (2, 4)))
    backup_up = gaussian(key_of[2], (N_DP, N_SECTION, N_TENSOR, ROWS_PIECE, FF), D ** -0.5, 0.09375, ((0, 2), (1, 16), (2, 4)))
    backup_down = gaussian(key_of[3], (N_DP, N_SECTION, N_TENSOR, ROWS_PIECE, FF), FF ** -0.5, 0.0625, ((0, 2), (1, 16), (2, 4)))
    norm_gain = jnp.clip(1.0 + 0.15 * jax.random.normal(key_of[4], (N_SECTION, D), jnp.float32), 0.25, 1.75)
    micro_batches = draw_micro_batches(jax.random.fold_in(key_of[8], 71), 0)
    failed_section = jax.random.randint(key_of[6], (1,), 0, N_SECTION * 65536).astype(jnp.int32)
    live_batches = jax.random.randint(key_of[7], (1,), 0, 65536 * (MB - MB // 2 + 1)).astype(jnp.int32)
    return dict(section_up=section_up, section_down=section_down, backup_up=backup_up, backup_down=backup_down, norm_gain=norm_gain, micro_batches=micro_batches, failed_section=failed_section, live_batches=live_batches)


def reference(section_up, section_down, backup_up, backup_down, norm_gain, micro_batches, failed_section, live_batches):
    failed = failed_section[0] % N_SECTION
    live_count = MB // 2 + live_batches[0] % (MB - MB // 2 + 1)
    spare_up = backup_up.reshape(D, FF)
    spare_down = backup_down.reshape(D, FF)
    batch_index = lax.broadcasted_iota(jnp.int32, (MB, 1, 1), 0)
    inputs = jnp.where(batch_index < live_count, micro_batches, jnp.zeros_like(micro_batches))
    state_rows = inputs.reshape(MB * TOKENS_MB, D)
    block_width = FF // N_TENSOR

    def one_section(carried, section_layer):
        up_weight, down_weight, gain_row, section_index = section_layer
        chosen_up = jnp.where(section_index == failed, spare_up, up_weight)
        chosen_down = jnp.where(section_index == failed, spare_down, down_weight)
        values = carried.astype(jnp.float32)
        mean_square = lax.optimization_barrier(jnp.mean(values * values, axis=1, keepdims=True))
        normed = (values * lax.rsqrt(mean_square + 1e-05) * gain_row).astype(jnp.bfloat16)
        hidden = jax.nn.silu(jnp.dot(normed, chosen_up, preferred_element_type=jnp.float32)).astype(jnp.bfloat16)
        down_total = jnp.zeros((carried.shape[0], D), jnp.float32)
        for block_index in range(N_TENSOR):
            lower = block_index * block_width
            block_term = lax.dot_general(hidden[:, lower:lower + block_width], chosen_down[:, lower:lower + block_width], (((1,), (1,)), ((), ())), preferred_element_type=jnp.float32)
            down_total = down_total + lax.optimization_barrier(block_term.astype(jnp.bfloat16)).astype(jnp.float32)
        return ((values + down_total).astype(jnp.bfloat16), None)
    indices = jnp.arange(N_SECTION, dtype=jnp.int32)
    final_rows, _ = lax.scan(one_section, state_rows, (section_up, section_down, norm_gain, indices))
    return final_rows.reshape(MB, TOKENS_MB, D)
```

```python
import functools

import jax
import jax.numpy as jnp
from jax import lax
from jax.experimental import pallas as pl
from jax.experimental.pallas import tpu as pltpu
from jax.sharding import PartitionSpec as P

MESH = pl.DeviceIdType.MESH
F32, BF16 = jnp.float32, jnp.bfloat16
M = 32
LAG_B, LAG_C = 1, 2
LOOK = 2


def wait_for(ref, sem):
    pltpu.make_async_copy(ref, ref, sem).wait()


def relay(
    n_section,
    n_tensor,
    up_ref,
    down_ref,
    gain_ref,
    mb_ref,
    out_ref,
    x_in,
    p_own,
    s_own,
    p_out,
    p_in,
    y_out,
    y_in,
    x_out,
    fin,
    x_recv,
    p_recv,
    y_recv,
    fin_recv,
    x_send,
    p_send,
    y_send,
    mb_send,
):
    s, t, d = lax.axis_index("section"), lax.axis_index("tensor"), lax.axis_index("dp")
    n_mb, tok = mb_ref.shape[0], mb_ref.shape[2]
    n_chunk, width = x_in.shape[0], x_in.shape[3]
    per_dp = tok // M
    half = n_tensor // 2
    features = n_tensor * width * 2
    hidden = down_ref.shape[1]
    cut = 1024

    def remote(src, dst, send, recv, where):
        return pltpu.make_async_remote_copy(src, dst, send, recv, device_id=where, device_id_type=MESH)

    def enter(b):
        for q in range(per_dp):
            c = (b * 2 + d) * per_dp + q
            src = mb_ref.at[b, :, pl.ds(q * M, M)]
            dst = x_in.at[c, pl.ds(lax.rem(t, half) * half, half)]
            for other in range(n_tensor):
                here = jnp.logical_and(t == other, d == t // half)

                @pl.when(here)
                def _():
                    pltpu.make_async_copy(src, dst, x_recv.at[c]).start()

                @pl.when(jnp.logical_not(here))
                def _():
                    remote(src, dst, mb_send.at[b], x_recv.at[c], (s, other, t // half)).start()

    def up_stage(c):
        wait_for(x_in.at[c], x_recv.at[c])
        squares = jnp.zeros((M, 1), F32)
        rows = []
        for j in range(n_tensor):
            values = x_in[c, j].astype(F32)
            squares = squares + jnp.sum(values * values, axis=1, keepdims=True)
            rows.append((values * gain_ref[:, j * width : (j + 1) * width]).astype(BF16))
        rows = jnp.concatenate(rows, axis=1)
        slot = lax.rem(c, LAG_B + 1)
        s_own[slot] = jnp.broadcast_to(squares, (M, 128))
        high = squares.astype(BF16)
        low = (squares - high.astype(F32)).astype(BF16)
        p_out[c, :, hidden : hidden + 64] = jnp.broadcast_to(high, (M, 64))
        p_out[c, :, hidden + 64 : hidden + 128] = jnp.broadcast_to(low, (M, 64))
        for lo, hi, end in ((0, cut, cut), (cut, hidden, hidden + 128)):
            terms = jnp.dot(rows, up_ref[:, lo:hi], preferred_element_type=F32)
            p_own[slot, :, lo:hi] = terms
            p_out[c, :, lo:hi] = terms.astype(BF16)
            remote(
                p_out.at[c, :, pl.ds(lo, end - lo)],
                p_in.at[c, :, pl.ds(lo, end - lo)],
                p_send.at[c],
                p_recv.at[c],
                (s, t, 1 - d),
            ).start()

    def down_stage(c):
        wait_for(p_in.at[c], p_recv.at[c])
        slot = lax.rem(c, LAG_B + 1)
        others = p_in[c, :, hidden : hidden + 1].astype(F32) + p_in[c, :, hidden + 64 : hidden + 65].astype(F32)
        scale = lax.rsqrt((s_own[slot, :, 0:1] + others) / features + 1e-05)
        v = (p_own[slot] + p_in[c, :, :hidden].astype(F32)) * scale
        act = (v / (1.0 + jnp.exp(-v))).astype(BF16)
        for step in (2, 1, 3, 0):
            to = lax.rem(t + step, n_tensor)
            y_out[c, step] = jnp.dot(act, down_ref[to], preferred_element_type=F32).astype(BF16)
            if step:
                remote(y_out.at[c, step], y_in.at[c, step - 1], y_send.at[c], y_recv.at[c], (s, to, d)).start()

    def sum_stage(c):
        wait_for(y_in.at[c], y_recv.at[c])
        total = x_in[c, t].astype(F32) + y_out[c, 0].astype(F32)
        for k in range(n_tensor - 1):
            total = total + y_in[c, k].astype(F32)
        x_out[c] = total.astype(BF16)

        @pl.when(s < n_section - 1)
        def _():
            for other in range(n_tensor):
                remote(x_out.at[c], x_in.at[c, t], x_send.at[c], x_recv.at[c], (s + 1, other, d)).start()

        @pl.when(s == n_section - 1)
        def _():
            b, to_d, q = final_place(c)
            to_t = half * d + t // half
            dst = fin.at[lax.rem(t, half), pl.ds(q * M, M)]
            here = at_home(b, to_d, to_t)

            @pl.when(here)
            def _():
                pltpu.make_async_copy(x_out.at[c], dst, fin_recv).start()

            @pl.when(jnp.logical_not(here))
            def _():
                remote(x_out.at[c], dst, x_send.at[c], fin_recv, (b, to_t, to_d)).start()

    def final_place(c):
        return c // (2 * per_dp), lax.rem(c // per_dp, 2), lax.rem(c, per_dp)

    def at_home(b, to_d, to_t):
        return jnp.logical_and(b == s, jnp.logical_and(to_d == d, to_t == t))

    @pl.when(s == 0)
    def _():
        for b in range(LOOK):
            enter(b)

    def tick(k, carry):
        ahead = k // (2 * per_dp) + LOOK

        @pl.when(jnp.logical_and(s == 0, jnp.logical_and(lax.rem(k, 2 * per_dp) == 0, ahead < n_mb)))
        def _():
            enter(ahead)

        @pl.when(k < n_chunk)
        def _():
            up_stage(k)

        @pl.when(jnp.logical_and(k >= LAG_B, k < n_chunk + LAG_B))
        def _():
            down_stage(k - LAG_B)

        @pl.when(k >= LAG_C)
        def _():
            sum_stage(k - LAG_C)

        return carry

    lax.fori_loop(0, n_chunk + LAG_C, tick, 0)

    def drain(c, carry):
        wait_for(p_out.at[c], p_send.at[c])
        wait_for(y_in.at[c], y_send.at[c])

        @pl.when(s < n_section - 1)
        def _():
            wait_for(x_in.at[c], x_send.at[c])

        b, to_d, q = final_place(c)
        sent = jnp.logical_not(at_home(b, to_d, half * d + t // half))

        @pl.when(jnp.logical_and(s == n_section - 1, sent))
        def _():
            wait_for(x_out.at[c], x_send.at[c])

        return carry

    lax.fori_loop(0, n_chunk, drain, 0)

    @pl.when(s == 0)
    def _():
        def drained(b, carry):
            mine = d == t // half

            @pl.when(mine)
            def _():
                wait_for(x_in.at[pl.ds(0, (n_tensor - 1) * per_dp), pl.ds(0, half)], mb_send.at[b])

            @pl.when(jnp.logical_not(mine))
            def _():
                wait_for(x_in.at[pl.ds(0, n_tensor * per_dp), pl.ds(0, half)], mb_send.at[b])

            return carry

        lax.fori_loop(0, n_mb, drained, 0)

    wait_for(fin, fin_recv)
    for k in range(half):
        out_ref[0, :, k * width : (k + 1) * width] = fin[k]


def pipelined(mesh, up, down, gain, entering):
    n_section, n_tensor = mesh.shape["section"], mesh.shape["tensor"]
    n_mb, half, tok, width = entering.shape
    n_chunk = n_mb * 2 * tok // M
    hidden = up.shape[1]
    dma = pltpu.SemaphoreType.DMA
    return pl.pallas_call(
        functools.partial(relay, n_section, n_tensor),
        out_shape=jax.ShapeDtypeStruct((1, tok, half * width), BF16),
        in_specs=[pl.BlockSpec(memory_space=pltpu.VMEM)] * 4,
        out_specs=pl.BlockSpec(memory_space=pltpu.VMEM),
        scratch_shapes=[
            pltpu.VMEM((n_chunk, n_tensor, M, width), BF16),
            pltpu.VMEM((LAG_B + 1, M, hidden), F32),
            pltpu.VMEM((LAG_B + 1, M, 128), F32),
            pltpu.VMEM((n_chunk, M, hidden + 128), BF16),
            pltpu.VMEM((n_chunk, M, hidden + 128), BF16),
            pltpu.VMEM((n_chunk, n_tensor, M, width), BF16),
            pltpu.VMEM((n_chunk, n_tensor - 1, M, width), BF16),
            pltpu.VMEM((n_chunk, M, width), BF16),
            pltpu.VMEM((half, tok, width), BF16),
            dma((n_chunk,)),
            dma((n_chunk,)),
            dma((n_chunk,)),
            dma,
            dma((n_chunk,)),
            dma((n_chunk,)),
            dma((n_chunk,)),
            dma((n_mb,)),
        ],
        compiler_params=pltpu.CompilerParams(has_side_effects=True, vmem_limit_bytes=60 * 1024 * 1024),
    )(up, down, gain, entering)


def sent_together(arrays, axis, split_dim, concat_dim, along):
    widths = [a.shape[along] for a in arrays]
    both = jnp.concatenate(arrays, axis=along)
    filled = lax.all_to_all(both, axis, split_axis=split_dim, concat_axis=concat_dim, tiled=True)
    return tuple(jnp.split(filled, [sum(widths[:k]) for k in range(1, len(widths))], axis=along))


def in_one_piece(arrays, axis, dim, along):
    ends, at = ([], 0)
    for a in arrays[:-1]:
        at += a.shape[along]
        ends.append(at)
    both = jnp.concatenate(arrays, axis=along)
    return tuple(jnp.split(lax.all_gather(both, axis, axis=dim, tiled=True), ends, axis=along))


def body(
    mesh,
    section_up,
    section_down,
    backup_up,
    backup_down,
    norm_gain,
    micro_batches,
    failed_section,
    live_batches,
):
    n_tensor = lax.axis_size("tensor")
    pieces = sent_together((backup_up, backup_down), "tensor", 4, 2, 0)
    gathered = in_one_piece((pieces[0], pieces[1]), "section", 1, 0)
    rows, block_width = section_up.shape[1], section_up.shape[2]
    rebuilt_up = gathered[0].reshape(-1, block_width)
    rebuilt_down = gathered[1].reshape(-1, block_width)
    is_failed = lax.axis_index("section") == failed_section[0] % lax.axis_size("section")
    mine_up = jnp.where(is_failed, rebuilt_up, section_up[0])
    mine_down = jnp.where(is_failed, rebuilt_down, section_down[0])
    mine_down = mine_down.reshape(n_tensor, rows // n_tensor, block_width).swapaxes(1, 2)
    gain = lax.dynamic_slice_in_dim(norm_gain, lax.axis_index("dp") * rows, rows, 1)
    batch_count, tok_rows, share = micro_batches.shape
    live_count = batch_count // 2 + live_batches[0] % (batch_count - batch_count // 2 + 1)
    is_live = jnp.arange(batch_count, dtype=jnp.int32)[:, None, None, None] < live_count
    width = rows // n_tensor
    entering = micro_batches.reshape(batch_count, tok_rows, share // width, width).swapaxes(1, 2)
    entering = jnp.where(is_live, entering, jnp.zeros_like(entering))
    return pipelined(mesh, mine_up, mine_down, gain, entering)


def solution(mesh):
    placed = (
        P("section", "dp", "tensor"),
        P("section", "dp", "tensor"),
        P("dp", "section", "tensor", None, None),
        P("dp", "section", "tensor", None, None),
        P("section", None),
        P(None, "dp", "tensor"),
        P(),
        P(),
    )
    return jax.shard_map(
        functools.partial(body, mesh),
        mesh=mesh,
        in_specs=placed,
        out_specs=P("section", "dp", "tensor"),
        check_vma=False,
    )
```

```python
import functools

import jax
import jax.numpy as jnp
from jax import lax
from jax.experimental import pallas as pl
from jax.experimental.pallas import tpu as pltpu
from jax.sharding import PartitionSpec as P

MESH = pl.DeviceIdType.MESH
F32, BF16 = jnp.float32, jnp.bfloat16
M = 32
LAG_B, LAG_C = 1, 2
BLOCK = 128
STEP = 2
LOOK = 2


def wait_for(ref, sem):
    pltpu.make_async_copy(ref, ref, sem).wait()


def kept_or_rebuilt(lost_ref, rebuilt, own, kind, j, per):
    lost = jnp.broadcast_to(lost_ref[0:1, :], (BLOCK, BLOCK))
    kept = 1 - lost
    for q in range(per):
        for i in range(rebuilt.shape[2]):
            cols = slice(i * BLOCK, (i + 1) * BLOCK)
            if kind == 0:
                at = (pl.ds(pl.multiple_of((j * per + q) * BLOCK, BLOCK), BLOCK), cols)
            else:
                at = (j, cols, slice(q * BLOCK, (q + 1) * BLOCK))
            own[at] = rebuilt[j * per + q, kind, i] * lost + own[at] * kept


def exchange(n_tensor, up_ref, down_ref, out_ref, got_up, got_down, sends, recvs, own):
    t = lax.axis_index("tensor")
    width = got_up.shape[2]

    def block(ref, to):
        return ref.at[:, pl.ds(pl.multiple_of(to * width, 128), width)]

    copies = []
    for step in (2, 1, 3):
        to = lax.rem(t + step, n_tensor)
        for k, (src, dst) in enumerate(((up_ref, got_up), (down_ref, got_down))):
            copy = pltpu.make_async_remote_copy(
                block(src, to),
                dst.at[t],
                sends.at[step - 1, k],
                recvs.at[step - 1, k],
                device_id={"tensor": to},
                device_id_type=MESH,
            )
            copy.start()
            copies.append(copy)
    for k, (src, dst) in enumerate(((up_ref, got_up), (down_ref, got_down))):
        copy = pltpu.make_async_copy(block(src, t), dst.at[t], own.at[k])
        copy.start()
        copies.append(copy)
    for copy in copies:
        copy.wait()
    for i in range(width // BLOCK):
        cols = slice(i * BLOCK, (i + 1) * BLOCK)
        out_ref[0, i] = jnp.concatenate([got_up[j, :, cols] for j in range(n_tensor)], axis=0)
        rows = jnp.concatenate([got_down[j, :, cols] for j in range(n_tensor)], axis=0)
        out_ref[1, i] = rows.astype(F32).T.astype(BF16)


def relay(
    n_section,
    n_tensor,
    own_up,
    own_down,
    spare,
    lost_ref,
    gain_ref,
    mb_ref,
    out_ref,
    up_ref,
    down_ref,
    rebuilt,
    x_in,
    p_own,
    s_own,
    p_out,
    p_in,
    y_part,
    y_out,
    y_in,
    x_out,
    fin,
    x_recv,
    p_recv,
    y_recv,
    fin_recv,
    x_send,
    p_send,
    y_send,
    mb_send,
    load_sem,
):
    s, t, d = lax.axis_index("section"), lax.axis_index("tensor"), lax.axis_index("dp")
    tok = mb_ref.shape[2]
    n_chunk, width = x_in.shape[0], x_in.shape[3]
    n_mb = n_chunk * M // (2 * tok)
    per_dp = tok // M
    half = n_tensor // 2
    features = n_tensor * width * 2
    hidden = down_ref.shape[1]
    cut = 1024

    def remote(src, dst, send, recv, where):
        return pltpu.make_async_remote_copy(src, dst, send, recv, device_id=where, device_id_type=MESH)

    def enter(b):
        for q in range(per_dp):
            c = (b * 2 + d) * per_dp + q
            src = mb_ref.at[b, :, pl.ds(q * M, M)]
            dst = x_in.at[c, pl.ds(lax.rem(t, half) * half, half)]
            for other in range(n_tensor):
                here = jnp.logical_and(t == other, d == t // half)

                @pl.when(here)
                def _():
                    pltpu.make_async_copy(src, dst, x_recv.at[c]).start()

                @pl.when(jnp.logical_not(here))
                def _():
                    remote(src, dst, mb_send.at[b], x_recv.at[c], (s, other, t // half)).start()

    def up_stage(c):
        wait_for(x_in.at[c], x_recv.at[c])
        squares = jnp.zeros((M, 1), F32)
        rows = []
        for j in range(n_tensor):
            values = x_in[c, j].astype(F32)
            squares = squares + jnp.sum(values * values, axis=1, keepdims=True)
            rows.append((values * gain_ref[:, j * width : (j + 1) * width]).astype(BF16))
        rows = jnp.concatenate(rows, axis=1)
        slot = lax.rem(c, LAG_B + 1)
        s_own[slot] = jnp.broadcast_to(squares, (M, 128))
        high = squares.astype(BF16)
        low = (squares - high.astype(F32)).astype(BF16)
        p_out[c, :, 0:64] = jnp.broadcast_to(high, (M, 64))
        p_out[c, :, 64:128] = jnp.broadcast_to(low, (M, 64))
        for k, (lo, hi, start) in enumerate(((0, cut, 0), (cut, hidden, cut + 128))):
            terms = jnp.dot(rows, up_ref[:, lo:hi], preferred_element_type=F32)
            p_own[slot, :, lo:hi] = terms
            p_out[c, :, lo + 128 : hi + 128] = terms.astype(BF16)
            piece = pl.ds(start, hi + 128 - start)
            remote(p_out.at[c, :, piece], p_in.at[c, :, piece], p_send.at[c], p_recv.at[c, k], (s, t, 1 - d)).start()

    def down_stage(c):
        slot = lax.rem(c, LAG_B + 1)
        wait_for(p_in.at[c, :, pl.ds(0, cut + 128)], p_recv.at[c, 0])
        others = p_in[c, :, 0:1].astype(F32) + p_in[c, :, 64:65].astype(F32)
        scale = lax.rsqrt((s_own[slot, :, 0:1] + others) / features + 1e-05)

        def silu_of(lo, hi):
            v = (p_own[slot, :, lo:hi] + p_in[c, :, lo + 128 : hi + 128].astype(F32)) * scale
            return (v / (1.0 + jnp.exp(-v))).astype(BF16)

        act = silu_of(0, cut)
        for step in (2, 1, 3, 0):
            to = lax.rem(t + step, n_tensor)
            y_part[step] = jnp.dot(act, down_ref[to, :cut], preferred_element_type=F32)
        wait_for(p_in.at[c, :, pl.ds(cut + 128, hidden - cut)], p_recv.at[c, 1])
        act = silu_of(cut, hidden)
        for step in (2, 1, 3, 0):
            to = lax.rem(t + step, n_tensor)
            whole = y_part[step] + jnp.dot(act, down_ref[to, cut:], preferred_element_type=F32)
            y_out[c, step] = whole.astype(BF16)
            if step:
                remote(y_out.at[c, step], y_in.at[c, step - 1], y_send.at[c], y_recv.at[c], (s, to, d)).start()

    def sum_stage(c):
        wait_for(y_in.at[c], y_recv.at[c])
        total = x_in[c, t].astype(F32) + y_out[c, 0].astype(F32)
        for k in range(n_tensor - 1):
            total = total + y_in[c, k].astype(F32)
        x_out[c] = total.astype(BF16)

        @pl.when(s < n_section - 1)
        def _():
            for step in (2, 1, 3, 0):
                to = lax.rem(t + step, n_tensor)
                remote(x_out.at[c], x_in.at[c, t], x_send.at[c], x_recv.at[c], (s + 1, to, d)).start()

        @pl.when(s == n_section - 1)
        def _():
            b, to_d, q = final_place(c)
            to_t = half * d + t // half
            dst = fin.at[lax.rem(t, half), pl.ds(q * M, M)]
            here = at_home(b, to_d, to_t)

            @pl.when(here)
            def _():
                pltpu.make_async_copy(x_out.at[c], dst, fin_recv).start()

            @pl.when(jnp.logical_not(here))
            def _():
                remote(x_out.at[c], dst, x_send.at[c], fin_recv, (b, to_t, to_d)).start()

    def final_place(c):
        return c // (2 * per_dp), lax.rem(c // per_dp, 2), lax.rem(c, per_dp)

    def at_home(b, to_d, to_t):
        return jnp.logical_and(b == s, jnp.logical_and(to_d == d, to_t == t))

    per = n_section // n_tensor

    def loads(kind, j):
        group = spare.at[pl.ds(j * per, per), kind], rebuilt.at[pl.ds(j * per, per), kind]
        if kind == 0:
            rows = pl.ds(pl.multiple_of(j * width, width), width)
            own = own_up.at[rows], up_ref.at[rows]
        else:
            own = own_down.at[j], down_ref.at[j]
        return [pltpu.make_async_copy(*pair, load_sem.at[kind, k, j]) for k, pair in enumerate((own, group))]

    def arrived(kind, own):
        def group(j, carry):
            for load in loads(kind, j):
                load.wait()
            kept_or_rebuilt(lost_ref, rebuilt, own, kind, j, per)
            return carry

        lax.fori_loop(0, n_tensor, group, 0)

    for kind in range(2):
        for j in range(n_tensor):
            for load in loads(kind, j):
                load.start()

    @pl.when(s == 0)
    def _():
        for b in range(LOOK):
            enter(b)

    arrived(0, up_ref)

    def tick(k, carry):
        ahead = k // (2 * per_dp) + LOOK

        @pl.when(jnp.logical_and(s == 0, jnp.logical_and(lax.rem(k, 2 * per_dp) == 0, ahead < n_mb)))
        def _():
            enter(ahead)

        @pl.when(k < n_chunk)
        def _():
            up_stage(k)

        @pl.when(k == LAG_B)
        def _():
            arrived(1, down_ref)

        @pl.when(jnp.logical_and(k >= LAG_B, k < n_chunk + LAG_B))
        def _():
            down_stage(k - LAG_B)

        @pl.when(k >= LAG_C)
        def _():
            sum_stage(k - LAG_C)

        return carry

    lax.fori_loop(0, n_chunk + LAG_C, tick, 0)

    def drain(c, carry):
        wait_for(p_out.at[c], p_send.at[c])
        wait_for(y_in.at[c], y_send.at[c])

        @pl.when(s < n_section - 1)
        def _():
            wait_for(x_in.at[c], x_send.at[c])

        b, to_d, q = final_place(c)
        sent = jnp.logical_not(at_home(b, to_d, half * d + t // half))

        @pl.when(jnp.logical_and(s == n_section - 1, sent))
        def _():
            wait_for(x_out.at[c], x_send.at[c])

        return carry

    lax.fori_loop(0, n_chunk, drain, 0)

    @pl.when(s == 0)
    def _():
        def drained(b, carry):
            mine = d == t // half

            @pl.when(mine)
            def _():
                wait_for(x_in.at[pl.ds(0, (n_tensor - 1) * per_dp), pl.ds(0, half)], mb_send.at[b])

            @pl.when(jnp.logical_not(mine))
            def _():
                wait_for(x_in.at[pl.ds(0, n_tensor * per_dp), pl.ds(0, half)], mb_send.at[b])

            return carry

        lax.fori_loop(0, n_mb, drained, 0)

    @pl.when(s < n_mb)
    def _():
        wait_for(fin, fin_recv)
        for k in range(half):
            out_ref[0, :, k * width : (k + 1) * width] = fin[k]

    @pl.when(s >= n_mb)
    def _():
        out_ref[...] = jnp.zeros_like(out_ref)


def pipelined(mesh, n_live, up, down, spare, lost, gain, entering):
    n_section, n_tensor = mesh.shape["section"], mesh.shape["tensor"]
    _, half, tok, width = entering.shape
    n_chunk = n_live * 2 * tok // M
    hidden = up.shape[1]
    dma = pltpu.SemaphoreType.DMA
    return pl.pallas_call(
        functools.partial(relay, n_section, n_tensor),
        out_shape=jax.ShapeDtypeStruct((1, tok, half * width), BF16),
        in_specs=[pl.BlockSpec(memory_space=pl.ANY)] * 3 + [pl.BlockSpec(memory_space=pltpu.VMEM)] * 3,
        out_specs=pl.BlockSpec(memory_space=pltpu.VMEM),
        scratch_shapes=[
            pltpu.VMEM(up.shape, BF16),
            pltpu.VMEM(down.shape, BF16),
            pltpu.VMEM(spare.shape, BF16),
            pltpu.VMEM((n_chunk, n_tensor, M, width), BF16),
            pltpu.VMEM((LAG_B + 1, M, hidden), F32),
            pltpu.VMEM((LAG_B + 1, M, 128), F32),
            pltpu.VMEM((n_chunk, M, hidden + 128), BF16),
            pltpu.VMEM((n_chunk, M, hidden + 128), BF16),
            pltpu.VMEM((n_tensor, M, width), F32),
            pltpu.VMEM((n_chunk, n_tensor, M, width), BF16),
            pltpu.VMEM((n_chunk, n_tensor - 1, M, width), BF16),
            pltpu.VMEM((n_chunk, M, width), BF16),
            pltpu.VMEM((half, tok, width), BF16),
            dma((n_chunk,)),
            dma((n_chunk, 2)),
            dma((n_chunk,)),
            dma,
            dma((n_chunk,)),
            dma((n_chunk,)),
            dma((n_chunk,)),
            dma((n_live,)),
            dma((2, 2, n_tensor)),
        ],
        compiler_params=pltpu.CompilerParams(has_side_effects=True, vmem_limit_bytes=60 * 1024 * 1024),
    )(up, down, spare, lost, gain, entering)


def by_columns(n_tensor, backup_up, backup_down):
    rows, width = backup_up.shape[0], backup_up.shape[1] // n_tensor
    dma = pltpu.SemaphoreType.DMA
    return pl.pallas_call(
        functools.partial(exchange, n_tensor),
        out_shape=jax.ShapeDtypeStruct((2, width // BLOCK, BLOCK, BLOCK), BF16),
        in_specs=[pl.BlockSpec(memory_space=pltpu.VMEM)] * 2,
        out_specs=pl.BlockSpec(memory_space=pltpu.VMEM),
        scratch_shapes=[
            pltpu.VMEM((n_tensor, rows, width), BF16),
            pltpu.VMEM((n_tensor, rows, width), BF16),
            dma((n_tensor - 1, 2)),
            dma((n_tensor - 1, 2)),
            dma((2,)),
        ],
        compiler_params=pltpu.CompilerParams(has_side_effects=True),
    )(backup_up, backup_down)


def body(
    mesh,
    section_up,
    section_down,
    backup_up,
    backup_down,
    norm_gain,
    micro_batches,
    failed_section,
    live_batches,
):
    n_tensor = lax.axis_size("tensor")
    pieces = by_columns(n_tensor, backup_up[0, 0, 0], backup_down[0, 0, 0])
    spare = lax.all_gather(pieces, "section", axis=0)
    rows, block_width = section_up.shape[1], section_up.shape[2]
    is_failed = lax.axis_index("section") == failed_section[0] % lax.axis_size("section")
    lost = jnp.broadcast_to(is_failed.astype(BF16), (16, BLOCK))
    own_down = section_down[0].reshape(n_tensor, rows // n_tensor, block_width).swapaxes(1, 2)
    gain = lax.dynamic_slice_in_dim(norm_gain, lax.axis_index("dp") * rows, rows, 1)
    batch_count, tok_rows, share = micro_batches.shape
    live_count = batch_count // 2 + live_batches[0] % (batch_count - batch_count // 2 + 1)
    is_live = jnp.arange(batch_count, dtype=jnp.int32)[:, None, None, None] < live_count
    width = rows // n_tensor
    entering = micro_batches.reshape(batch_count, tok_rows, share // width, width).swapaxes(1, 2)
    entering = jnp.where(is_live, entering, jnp.zeros_like(entering))
    fewest = batch_count // 2
    sizes = list(range(fewest, batch_count, STEP)) + [batch_count]
    return lax.switch(
        (live_count - fewest + STEP - 1) // STEP,
        [functools.partial(pipelined, mesh, n_live) for n_live in sizes],
        section_up[0],
        own_down,
        spare,
        lost,
        gain,
        entering,
    )


def solution(mesh):
    placed = (
        P("section", "dp", "tensor"),
        P("section", "dp", "tensor"),
        P("dp", "section", "tensor", None, None),
        P("dp", "section", "tensor", None, None),
        P("section", None),
        P(None, "dp", "tensor"),
        P(),
        P(),
    )
    return jax.shard_map(
        functools.partial(body, mesh),
        mesh=mesh,
        in_specs=placed,
        out_specs=P("section", "dp", "tensor"),
        check_vma=False,
    )
```

```python
import functools

import jax
import jax.numpy as jnp
from jax import lax
from jax.experimental import pallas as pl
from jax.experimental.pallas import tpu as pltpu
from jax.sharding import PartitionSpec as P

MESH = pl.DeviceIdType.MESH
F32, BF16 = jnp.float32, jnp.bfloat16
M = 32
LAG_B, LAG_C = 1, 2
BLOCK = 128
STEP = 2
LOOK = 2


def wait_for(ref, sem):
    pltpu.make_async_copy(ref, ref, sem).wait()


def kept_or_rebuilt(lost_ref, rebuilt, own, kind, j, per):
    lost = jnp.broadcast_to(lost_ref[0:1, :], (BLOCK, BLOCK))
    kept = 1 - lost
    for q in range(per):
        for i in range(rebuilt.shape[2]):
            cols = slice(i * BLOCK, (i + 1) * BLOCK)
            if kind == 0:
                at = (pl.ds(pl.multiple_of((j * per + q) * BLOCK, BLOCK), BLOCK), cols)
            else:
                at = (j, cols, slice(q * BLOCK, (q + 1) * BLOCK))
            own[at] = rebuilt[j * per + q, kind, i] * lost + own[at] * kept


def exchange(n_tensor, up_ref, down_ref, out_ref, got_up, got_down, sends, recvs, own):
    t = lax.axis_index("tensor")
    width = got_up.shape[2]

    def block(ref, to):
        return ref.at[:, pl.ds(pl.multiple_of(to * width, 128), width)]

    copies = []
    for step in (2, 1, 3):
        to = lax.rem(t + step, n_tensor)
        for k, (src, dst) in enumerate(((up_ref, got_up), (down_ref, got_down))):
            copy = pltpu.make_async_remote_copy(
                block(src, to),
                dst.at[t],
                sends.at[step - 1, k],
                recvs.at[step - 1, k],
                device_id={"tensor": to},
                device_id_type=MESH,
            )
            copy.start()
            copies.append(copy)
    for k, (src, dst) in enumerate(((up_ref, got_up), (down_ref, got_down))):
        copy = pltpu.make_async_copy(block(src, t), dst.at[t], own.at[k])
        copy.start()
        copies.append(copy)
    for copy in copies:
        copy.wait()
    for i in range(width // BLOCK):
        cols = slice(i * BLOCK, (i + 1) * BLOCK)
        out_ref[0, i] = jnp.concatenate([got_up[j, :, cols] for j in range(n_tensor)], axis=0)
        rows = jnp.concatenate([got_down[j, :, cols] for j in range(n_tensor)], axis=0)
        out_ref[1, i] = rows.astype(F32).T.astype(BF16)


def relay(
    n_section,
    n_tensor,
    own_up,
    own_down,
    spare,
    lost_ref,
    gain_ref,
    mb_ref,
    out_ref,
    up_ref,
    down_ref,
    rebuilt,
    x_in,
    p_own,
    s_own,
    p_out,
    p_in,
    y_part,
    y_out,
    y_in,
    x_out,
    fin,
    x_recv,
    p_recv,
    y_recv,
    fin_recv,
    x_send,
    p_send,
    y_send,
    mb_send,
    z_send,
    z_recv,
    load_sem,
):
    s, t, d = lax.axis_index("section"), lax.axis_index("tensor"), lax.axis_index("dp")
    tok = mb_ref.shape[2]
    n_chunk, width = x_in.shape[0], x_in.shape[3]
    n_mb = n_chunk * M // (2 * tok)
    per_dp = tok // M
    half = n_tensor // 2
    features = n_tensor * width * 2
    hidden = down_ref.shape[1]
    cut = 1024
    on_chip = lax.rem(s, 2) == 0
    off_chip = jnp.logical_and(lax.rem(s, 2) == 1, s < n_section - 1)

    def remote(src, dst, send, recv, where):
        return pltpu.make_async_remote_copy(src, dst, send, recv, device_id=where, device_id_type=MESH)

    def enter(b):
        for q in range(per_dp):
            c = (b * 2 + d) * per_dp + q
            src = mb_ref.at[b, :, pl.ds(q * M, M)]
            dst = x_in.at[c, pl.ds(lax.rem(t, half) * half, half)]
            for other in range(n_tensor):
                here = jnp.logical_and(t == other, d == t // half)

                @pl.when(here)
                def _():
                    pltpu.make_async_copy(src, dst, x_recv.at[c]).start()

                @pl.when(jnp.logical_not(here))
                def _():
                    remote(src, dst, mb_send.at[b], x_recv.at[c], (s, other, t // half)).start()

    def up_stage(c):
        wait_for(x_in.at[c], x_recv.at[c])
        squares = jnp.zeros((M, 1), F32)
        rows = []
        for j in range(n_tensor):
            values = x_in[c, j].astype(F32)
            squares = squares + jnp.sum(values * values, axis=1, keepdims=True)
            at = pl.multiple_of((d * n_tensor + j) * width, BLOCK)
            rows.append((values * gain_ref[:, pl.ds(at, width)]).astype(BF16))
        rows = jnp.concatenate(rows, axis=1)
        slot = lax.rem(c, LAG_B + 1)
        s_own[slot] = jnp.broadcast_to(squares, (M, 128))
        high = squares.astype(BF16)
        low = (squares - high.astype(F32)).astype(BF16)
        p_out[c, :, 0:64] = jnp.broadcast_to(high, (M, 64))
        p_out[c, :, 64:128] = jnp.broadcast_to(low, (M, 64))
        for k, (lo, hi, start) in enumerate(((0, cut, 0), (cut, hidden, cut + 128))):
            terms = jnp.dot(rows, up_ref[:, lo:hi], preferred_element_type=F32)
            p_own[slot, :, lo:hi] = terms
            p_out[c, :, lo + 128 : hi + 128] = terms.astype(BF16)
            piece = pl.ds(start, hi + 128 - start)
            remote(p_out.at[c, :, piece], p_in.at[c, :, piece], p_send.at[c], p_recv.at[c, k], (s, t, 1 - d)).start()

    def down_stage(c):
        slot = lax.rem(c, LAG_B + 1)
        wait_for(p_in.at[c, :, pl.ds(0, cut + 128)], p_recv.at[c, 0])
        others = p_in[c, :, 0:1].astype(F32) + p_in[c, :, 64:65].astype(F32)
        scale = lax.rsqrt((s_own[slot, :, 0:1] + others) / features + 1e-05)

        def silu_of(lo, hi):
            v = (p_own[slot, :, lo:hi] + p_in[c, :, lo + 128 : hi + 128].astype(F32)) * scale
            return (v / (1.0 + jnp.exp(-v))).astype(BF16)

        act = silu_of(0, cut)
        for step in (2, 1, 3, 0):
            to = lax.rem(t + step, n_tensor)
            y_part[step] = jnp.dot(act, down_ref[to, :cut], preferred_element_type=F32)
        wait_for(p_in.at[c, :, pl.ds(cut + 128, hidden - cut)], p_recv.at[c, 1])
        act = silu_of(cut, hidden)
        for step in (2, 1, 3, 0):
            to = lax.rem(t + step, n_tensor)
            whole = y_part[step] + jnp.dot(act, down_ref[to, cut:], preferred_element_type=F32)
            y_out[c, step] = whole.astype(BF16)
            if step:
                remote(y_out.at[c, step], y_in.at[c, step - 1], y_send.at[c], y_recv.at[c], (s, to, d)).start()

    def sum_stage(c):
        wait_for(y_in.at[c], y_recv.at[c])
        total = x_in[c, t].astype(F32) + y_out[c, 0].astype(F32)
        for k in range(n_tensor - 1):
            total = total + y_in[c, k].astype(F32)
        x_out[c, t] = total.astype(BF16)
        mine = x_out.at[c, t]

        @pl.when(on_chip)
        def _():
            for step in (2, 1, 3, 0):
                to = lax.rem(t + step, n_tensor)
                remote(mine, x_in.at[c, t], x_send.at[c], x_recv.at[c], (s + 1, to, d)).start()

        @pl.when(off_chip)
        def _():
            for step in (2, 1, 3):
                to = lax.rem(t + step, n_tensor)
                remote(mine, mine, z_send.at[c], z_recv.at[c], (s, to, d)).start()

        @pl.when(s == n_section - 1)
        def _():
            b, to_d, q = final_place(c)
            to_t = half * d + t // half
            dst = fin.at[lax.rem(t, half), pl.ds(q * M, M)]
            here = at_home(b, to_d, to_t)

            @pl.when(here)
            def _():
                pltpu.make_async_copy(mine, dst, fin_recv).start()

            @pl.when(jnp.logical_not(here))
            def _():
                remote(mine, dst, x_send.at[c], fin_recv, (b, to_t, to_d)).start()

    def hand_on(c):
        wait_for(y_in.at[c], z_recv.at[c])
        remote(x_out.at[c], x_in.at[c], x_send.at[c], x_recv.at[c], (s + 1, t, d)).start()

    def final_place(c):
        return c // (2 * per_dp), lax.rem(c // per_dp, 2), lax.rem(c, per_dp)

    def at_home(b, to_d, to_t):
        return jnp.logical_and(b == s, jnp.logical_and(to_d == d, to_t == t))

    per = n_section // n_tensor

    def loads(kind, j):
        group = spare.at[pl.ds(j * per, per), kind], rebuilt.at[pl.ds(j * per, per), kind]
        if kind == 0:
            rows = pl.ds(pl.multiple_of(j * width, width), width)
            own = own_up.at[rows], up_ref.at[rows]
        else:
            own = own_down.at[j], down_ref.at[j]
        return [pltpu.make_async_copy(*pair, load_sem.at[kind, k, j]) for k, pair in enumerate((own, group))]

    def arrived(kind, own):
        def group(j, carry):
            for load in loads(kind, j):
                load.wait()
            kept_or_rebuilt(lost_ref, rebuilt, own, kind, j, per)
            return carry

        lax.fori_loop(0, n_tensor, group, 0)

    for kind in range(2):
        for j in range(n_tensor):
            for load in loads(kind, j):
                load.start()

    @pl.when(s == 0)
    def _():
        for b in range(LOOK):
            enter(b)

    arrived(0, up_ref)

    def tick(k, carry):
        ahead = k // (2 * per_dp) + LOOK

        @pl.when(jnp.logical_and(s == 0, jnp.logical_and(lax.rem(k, 2 * per_dp) == 0, ahead < n_mb)))
        def _():
            enter(ahead)

        @pl.when(k < n_chunk)
        def _():
            up_stage(k)

        @pl.when(k == LAG_B)
        def _():
            arrived(1, down_ref)

        @pl.when(jnp.logical_and(k >= LAG_B, k < n_chunk + LAG_B))
        def _():
            down_stage(k - LAG_B)

        @pl.when(jnp.logical_and(off_chip, k >= LAG_C + 1))
        def _():
            hand_on(k - LAG_C - 1)

        @pl.when(jnp.logical_and(k >= LAG_C, k < n_chunk + LAG_C))
        def _():
            sum_stage(k - LAG_C)

        return carry

    lax.fori_loop(0, n_chunk + LAG_C + 1, tick, 0)

    def drain(c, carry):
        wait_for(p_out.at[c], p_send.at[c])
        wait_for(y_in.at[c], y_send.at[c])

        @pl.when(s < n_section - 1)
        def _():
            wait_for(x_in.at[c], x_send.at[c])

        @pl.when(off_chip)
        def _():
            wait_for(y_in.at[c], z_send.at[c])

        b, to_d, q = final_place(c)
        sent = jnp.logical_not(at_home(b, to_d, half * d + t // half))

        @pl.when(jnp.logical_and(s == n_section - 1, sent))
        def _():
            wait_for(x_out.at[c, t], x_send.at[c])

        return carry

    lax.fori_loop(0, n_chunk, drain, 0)

    @pl.when(s == 0)
    def _():
        def drained(b, carry):
            mine = d == t // half

            @pl.when(mine)
            def _():
                wait_for(x_in.at[pl.ds(0, (n_tensor - 1) * per_dp), pl.ds(0, half)], mb_send.at[b])

            @pl.when(jnp.logical_not(mine))
            def _():
                wait_for(x_in.at[pl.ds(0, n_tensor * per_dp), pl.ds(0, half)], mb_send.at[b])

            return carry

        lax.fori_loop(0, n_mb, drained, 0)

    @pl.when(s < n_mb)
    def _():
        wait_for(fin, fin_recv)
        for k in range(half):
            out_ref[0, :, k * width : (k + 1) * width] = fin[k]

    @pl.when(s >= n_mb)
    def _():
        out_ref[...] = jnp.zeros_like(out_ref)


def pipelined(mesh, n_live, up, down, spare, lost, gain, entering):
    n_section, n_tensor = mesh.shape["section"], mesh.shape["tensor"]
    _, half, tok, width = entering.shape
    n_chunk = n_live * 2 * tok // M
    hidden = up.shape[1]
    dma = pltpu.SemaphoreType.DMA
    return pl.pallas_call(
        functools.partial(relay, n_section, n_tensor),
        out_shape=jax.ShapeDtypeStruct((1, tok, half * width), BF16),
        in_specs=[pl.BlockSpec(memory_space=pl.ANY)] * 3 + [pl.BlockSpec(memory_space=pltpu.VMEM)] * 3,
        out_specs=pl.BlockSpec(memory_space=pltpu.VMEM),
        scratch_shapes=[
            pltpu.VMEM(up.shape, BF16),
            pltpu.VMEM(down.shape, BF16),
            pltpu.VMEM(spare.shape, BF16),
            pltpu.VMEM((n_chunk, n_tensor, M, width), BF16),
            pltpu.VMEM((LAG_B + 1, M, hidden), F32),
            pltpu.VMEM((LAG_B + 1, M, 128), F32),
            pltpu.VMEM((n_chunk, M, hidden + 128), BF16),
            pltpu.VMEM((n_chunk, M, hidden + 128), BF16),
            pltpu.VMEM((n_tensor, M, width), F32),
            pltpu.VMEM((n_chunk, n_tensor, M, width), BF16),
            pltpu.VMEM((n_chunk, n_tensor - 1, M, width), BF16),
            pltpu.VMEM((n_chunk, n_tensor, M, width), BF16),
            pltpu.VMEM((half, tok, width), BF16),
            dma((n_chunk,)),
            dma((n_chunk, 2)),
            dma((n_chunk,)),
            dma,
            dma((n_chunk,)),
            dma((n_chunk,)),
            dma((n_chunk,)),
            dma((n_live,)),
            dma((n_chunk,)),
            dma((n_chunk,)),
            dma((2, 2, n_tensor)),
        ],
        compiler_params=pltpu.CompilerParams(has_side_effects=True, vmem_limit_bytes=60 * 1024 * 1024),
    )(up, down, spare, lost, gain, entering)


def by_columns(n_tensor, backup_up, backup_down):
    rows, width = backup_up.shape[0], backup_up.shape[1] // n_tensor
    dma = pltpu.SemaphoreType.DMA
    return pl.pallas_call(
        functools.partial(exchange, n_tensor),
        out_shape=jax.ShapeDtypeStruct((2, width // BLOCK, BLOCK, BLOCK), BF16),
        in_specs=[pl.BlockSpec(memory_space=pltpu.VMEM)] * 2,
        out_specs=pl.BlockSpec(memory_space=pltpu.VMEM),
        scratch_shapes=[
            pltpu.VMEM((n_tensor, rows, width), BF16),
            pltpu.VMEM((n_tensor, rows, width), BF16),
            dma((n_tensor - 1, 2)),
            dma((n_tensor - 1, 2)),
            dma((2,)),
        ],
        compiler_params=pltpu.CompilerParams(has_side_effects=True),
    )(backup_up, backup_down)


def turned(n_tensor, down):
    rows, hidden = down.shape
    width = rows // n_tensor

    def turn(down_ref, out_ref):
        out_ref[0] = down_ref[...].astype(F32).T.astype(BF16)

    return pl.pallas_call(
        turn,
        grid=(n_tensor, hidden // BLOCK),
        out_shape=jax.ShapeDtypeStruct((n_tensor, hidden, width), BF16),
        in_specs=[pl.BlockSpec((width, BLOCK), lambda j, i: (j, i))],
        out_specs=pl.BlockSpec((1, BLOCK, width), lambda j, i: (j, i, 0)),
        cost_estimate=pl.CostEstimate(flops=0, bytes_accessed=16 * rows * hidden, transcendentals=0),
    )(down)


def cut_up(micro_batches, live_count, width):
    count, rows, share = micro_batches.shape

    def cut(live_ref, mb_ref, out_ref):
        factor = (pl.program_id(0) < live_ref[0]).astype(F32)
        for k in range(share // width):
            out_ref[0, k] = (mb_ref[0, :, k * width : (k + 1) * width].astype(F32) * factor).astype(BF16)

    return pl.pallas_call(
        cut,
        grid=(count,),
        out_shape=jax.ShapeDtypeStruct((count, share // width, rows, width), BF16),
        in_specs=[
            pl.BlockSpec(memory_space=pltpu.SMEM),
            pl.BlockSpec((1, rows, share), lambda b: (b, 0, 0)),
        ],
        out_specs=pl.BlockSpec((1, share // width, rows, width), lambda b: (b, 0, 0, 0)),
        cost_estimate=pl.CostEstimate(flops=0, bytes_accessed=16 * count * rows * share, transcendentals=0),
    )(live_count.reshape(1), micro_batches)


def body(
    mesh,
    section_up,
    section_down,
    backup_up,
    backup_down,
    norm_gain,
    micro_batches,
    failed_section,
    live_batches,
):
    n_tensor = lax.axis_size("tensor")
    pieces = by_columns(n_tensor, backup_up[0, 0, 0], backup_down[0, 0, 0])
    spare = lax.all_gather(pieces, "section", axis=0)
    rows = section_up.shape[1]
    is_failed = lax.axis_index("section") == failed_section[0] % lax.axis_size("section")
    lost = jnp.broadcast_to(is_failed.astype(BF16), (16, BLOCK))
    own_down = turned(n_tensor, section_down[0])
    batch_count = micro_batches.shape[0]
    live_count = batch_count // 2 + live_batches[0] % (batch_count - batch_count // 2 + 1)
    entering = cut_up(micro_batches, live_count, rows // n_tensor)
    fewest = batch_count // 2
    sizes = list(range(fewest, batch_count, STEP)) + [batch_count]
    return lax.switch(
        (live_count - fewest + STEP - 1) // STEP,
        [functools.partial(pipelined, mesh, n_live) for n_live in sizes],
        section_up[0],
        own_down,
        spare,
        lost,
        norm_gain,
        entering,
    )


def solution(mesh):
    placed = (
        P("section", "dp", "tensor"),
        P("section", "dp", "tensor"),
        P("dp", "section", "tensor", None, None),
        P("dp", "section", "tensor", None, None),
        P("section", None),
        P(None, "dp", "tensor"),
        P(),
        P(),
    )
    return jax.shard_map(
        functools.partial(body, mesh),
        mesh=mesh,
        in_specs=placed,
        out_specs=P("section", "dp", "tensor"),
        check_vma=False,
    )
```

```python
import functools

import jax
import jax.numpy as jnp
from jax import lax
from jax.experimental import pallas as pl
from jax.experimental.pallas import tpu as pltpu
from jax.sharding import PartitionSpec as P

MESH = pl.DeviceIdType.MESH
F32, BF16 = jnp.float32, jnp.bfloat16
M = 32
LAG_B, LAG_C = 1, 2
BLOCK = 128
STEP = 2
LOOK = 2


def wait_for(ref, sem):
    pltpu.make_async_copy(ref, ref, sem).wait()


def kept_or_rebuilt(lost_ref, rebuilt, own, kind, j, per):
    lost = jnp.broadcast_to(lost_ref[0:1, :], (BLOCK, BLOCK))
    kept = 1 - lost
    for q in range(per):
        for i in range(rebuilt.shape[2]):
            cols = slice(i * BLOCK, (i + 1) * BLOCK)
            if kind == 0:
                at = (pl.ds(pl.multiple_of((j * per + q) * BLOCK, BLOCK), BLOCK), cols)
            else:
                at = (j, cols, slice(q * BLOCK, (q + 1) * BLOCK))
            own[at] = rebuilt[j * per + q, kind, i] * lost + own[at] * kept


def exchange(n_tensor, up_ref, down_ref, out_ref, got_up, got_down, sends, recvs, own):
    t = lax.axis_index("tensor")
    width = got_up.shape[2]

    def block(ref, to):
        return ref.at[:, pl.ds(pl.multiple_of(to * width, 128), width)]

    copies = []
    for step in (2, 1, 3):
        to = lax.rem(t + step, n_tensor)
        for k, (src, dst) in enumerate(((up_ref, got_up), (down_ref, got_down))):
            copy = pltpu.make_async_remote_copy(
                block(src, to),
                dst.at[t],
                sends.at[step - 1, k],
                recvs.at[step - 1, k],
                device_id={"tensor": to},
                device_id_type=MESH,
            )
            copy.start()
            copies.append(copy)
    for k, (src, dst) in enumerate(((up_ref, got_up), (down_ref, got_down))):
        copy = pltpu.make_async_copy(block(src, t), dst.at[t], own.at[k])
        copy.start()
        copies.append(copy)
    for copy in copies:
        copy.wait()
    for i in range(width // BLOCK):
        cols = slice(i * BLOCK, (i + 1) * BLOCK)
        out_ref[0, i] = jnp.concatenate([got_up[j, :, cols] for j in range(n_tensor)], axis=0)
        rows = jnp.concatenate([got_down[j, :, cols] for j in range(n_tensor)], axis=0)
        out_ref[1, i] = rows.astype(F32).T.astype(BF16)


def relay(
    n_section,
    n_tensor,
    own_up,
    own_down,
    spare,
    lost_ref,
    gain_ref,
    mb_ref,
    out_ref,
    up_ref,
    down_ref,
    rebuilt,
    x_in,
    p_own,
    s_own,
    p_out,
    p_in,
    y_part,
    y_out,
    y_in,
    x_out,
    fin,
    x_recv,
    p_recv,
    y_recv,
    fin_recv,
    x_send,
    p_send,
    y_send,
    mb_send,
    load_sem,
):
    s, t, d = lax.axis_index("section"), lax.axis_index("tensor"), lax.axis_index("dp")
    tok = mb_ref.shape[2]
    n_chunk, width = x_in.shape[0], x_in.shape[3]
    n_mb = n_chunk * M // (2 * tok)
    per_dp = tok // M
    half = n_tensor // 2
    features = n_tensor * width * 2
    hidden = down_ref.shape[1]
    cut = 1024

    def remote(src, dst, send, recv, where):
        return pltpu.make_async_remote_copy(src, dst, send, recv, device_id=where, device_id_type=MESH)

    def enter(b):
        for q in range(per_dp):
            c = (b * 2 + d) * per_dp + q
            src = mb_ref.at[b, :, pl.ds(q * M, M)]
            dst = x_in.at[c, pl.ds(lax.rem(t, half) * half, half)]
            for other in range(n_tensor):
                here = jnp.logical_and(t == other, d == t // half)

                @pl.when(here)
                def _():
                    pltpu.make_async_copy(src, dst, x_recv.at[c]).start()

                @pl.when(jnp.logical_not(here))
                def _():
                    remote(src, dst, mb_send.at[b], x_recv.at[c], (s, other, t // half)).start()

    def up_stage(c):
        wait_for(x_in.at[c], x_recv.at[c])
        squares = jnp.zeros((M, 1), F32)
        rows = []
        for j in range(n_tensor):
            values = x_in[c, j].astype(F32)
            squares = squares + jnp.sum(values * values, axis=1, keepdims=True)
            at = pl.multiple_of((d * n_tensor + j) * width, BLOCK)
            rows.append((values * gain_ref[:, pl.ds(at, width)]).astype(BF16))
        rows = jnp.concatenate(rows, axis=1)
        slot = lax.rem(c, LAG_B + 1)
        s_own[slot] = jnp.broadcast_to(squares, (M, 128))
        high = squares.astype(BF16)
        low = (squares - high.astype(F32)).astype(BF16)
        p_out[c, :, 0:64] = jnp.broadcast_to(high, (M, 64))
        p_out[c, :, 64:128] = jnp.broadcast_to(low, (M, 64))
        for k, (lo, hi, start) in enumerate(((0, cut, 0), (cut, hidden, cut + 128))):
            terms = jnp.dot(rows, up_ref[:, lo:hi], preferred_element_type=F32)
            p_own[slot, :, lo:hi] = terms
            p_out[c, :, lo + 128 : hi + 128] = terms.astype(BF16)
            piece = pl.ds(start, hi + 128 - start)
            remote(p_out.at[c, :, piece], p_in.at[c, :, piece], p_send.at[c], p_recv.at[c, k], (s, t, 1 - d)).start()

    def down_stage(c):
        slot = lax.rem(c, LAG_B + 1)
        wait_for(p_in.at[c, :, pl.ds(0, cut + 128)], p_recv.at[c, 0])
        others = p_in[c, :, 0:1].astype(F32) + p_in[c, :, 64:65].astype(F32)
        scale = lax.rsqrt((s_own[slot, :, 0:1] + others) / features + 1e-05)

        def silu_of(lo, hi):
            v = (p_own[slot, :, lo:hi] + p_in[c, :, lo + 128 : hi + 128].astype(F32)) * scale
            return (v / (1.0 + jnp.exp(-v))).astype(BF16)

        act = silu_of(0, cut)
        for step in (2, 1, 3, 0):
            to = lax.rem(t + step, n_tensor)
            y_part[step] = jnp.dot(act, down_ref[to, :cut], preferred_element_type=F32)
        wait_for(p_in.at[c, :, pl.ds(cut + 128, hidden - cut)], p_recv.at[c, 1])
        act = silu_of(cut, hidden)
        for step in (2, 1, 3, 0):
            to = lax.rem(t + step, n_tensor)
            whole = y_part[step] + jnp.dot(act, down_ref[to, cut:], preferred_element_type=F32)
            y_out[c, step] = whole.astype(BF16)
            if step:
                remote(y_out.at[c, step], y_in.at[c, step - 1], y_send.at[c], y_recv.at[c], (s, to, d)).start()

    def sum_stage(c):
        wait_for(y_in.at[c], y_recv.at[c])
        total = x_in[c, t].astype(F32) + y_out[c, 0].astype(F32)
        for k in range(n_tensor - 1):
            total = total + y_in[c, k].astype(F32)
        x_out[c] = total.astype(BF16)
        mine = x_out.at[c]

        @pl.when(s < n_section - 1)
        def _():
            for step in (2, 1, 3, 0):
                to = lax.rem(t + step, n_tensor)
                remote(mine, x_in.at[c, t], x_send.at[c], x_recv.at[c], (s + 1, to, d)).start()


        @pl.when(s == n_section - 1)
        def _():
            b, to_d, q = final_place(c)
            to_t = half * d + t // half
            dst = fin.at[lax.rem(t, half), pl.ds(q * M, M)]
            here = at_home(b, to_d, to_t)

            @pl.when(here)
            def _():
                pltpu.make_async_copy(mine, dst, fin_recv).start()

            @pl.when(jnp.logical_not(here))
            def _():
                remote(mine, dst, x_send.at[c], fin_recv, (b, to_t, to_d)).start()

    def final_place(c):
        return c // (2 * per_dp), lax.rem(c // per_dp, 2), lax.rem(c, per_dp)

    def at_home(b, to_d, to_t):
        return jnp.logical_and(b == s, jnp.logical_and(to_d == d, to_t == t))

    per = n_section // n_tensor

    def loads(kind, j):
        group = spare.at[pl.ds(j * per, per), kind], rebuilt.at[pl.ds(j * per, per), kind]
        if kind == 0:
            rows = pl.ds(pl.multiple_of(j * width, width), width)
            own = own_up.at[rows], up_ref.at[rows]
        else:
            own = own_down.at[j], down_ref.at[j]
        return [pltpu.make_async_copy(*pair, load_sem.at[kind, k, j]) for k, pair in enumerate((own, group))]

    def arrived(kind, own):
        def group(j, carry):
            for load in loads(kind, j):
                load.wait()
            kept_or_rebuilt(lost_ref, rebuilt, own, kind, j, per)
            return carry

        lax.fori_loop(0, n_tensor, group, 0)

    for kind in range(2):
        for j in range(n_tensor):
            for load in loads(kind, j):
                load.start()

    @pl.when(s == 0)
    def _():
        for b in range(LOOK):
            enter(b)

    arrived(0, up_ref)

    def tick(k, carry):
        ahead = k // (2 * per_dp) + LOOK

        @pl.when(jnp.logical_and(s == 0, jnp.logical_and(lax.rem(k, 2 * per_dp) == 0, ahead < n_mb)))
        def _():
            enter(ahead)

        @pl.when(k < n_chunk)
        def _():
            up_stage(k)

        @pl.when(k == LAG_B)
        def _():
            arrived(1, down_ref)

        @pl.when(jnp.logical_and(k >= LAG_B, k < n_chunk + LAG_B))
        def _():
            down_stage(k - LAG_B)

        @pl.when(k >= LAG_C)
        def _():
            sum_stage(k - LAG_C)

        return carry

    lax.fori_loop(0, n_chunk + LAG_C, tick, 0)

    def drain(c, carry):
        wait_for(p_out.at[c], p_send.at[c])
        wait_for(y_in.at[c], y_send.at[c])

        @pl.when(s < n_section - 1)
        def _():
            wait_for(x_in.at[c], x_send.at[c])

        b, to_d, q = final_place(c)
        sent = jnp.logical_not(at_home(b, to_d, half * d + t // half))

        @pl.when(jnp.logical_and(s == n_section - 1, sent))
        def _():
            wait_for(x_out.at[c], x_send.at[c])

        return carry

    lax.fori_loop(0, n_chunk, drain, 0)

    @pl.when(s == 0)
    def _():
        def drained(b, carry):
            mine = d == t // half

            @pl.when(mine)
            def _():
                wait_for(x_in.at[pl.ds(0, (n_tensor - 1) * per_dp), pl.ds(0, half)], mb_send.at[b])

            @pl.when(jnp.logical_not(mine))
            def _():
                wait_for(x_in.at[pl.ds(0, n_tensor * per_dp), pl.ds(0, half)], mb_send.at[b])

            return carry

        lax.fori_loop(0, n_mb, drained, 0)

    @pl.when(s < n_mb)
    def _():
        wait_for(fin, fin_recv)
        for k in range(half):
            out_ref[0, :, k * width : (k + 1) * width] = fin[k]

    @pl.when(s >= n_mb)
    def _():
        out_ref[...] = jnp.zeros_like(out_ref)


def pipelined(mesh, n_live, up, down, spare, lost, gain, entering):
    n_section, n_tensor = mesh.shape["section"], mesh.shape["tensor"]
    _, half, tok, width = entering.shape
    n_chunk = n_live * 2 * tok // M
    hidden = up.shape[1]
    dma = pltpu.SemaphoreType.DMA
    return pl.pallas_call(
        functools.partial(relay, n_section, n_tensor),
        out_shape=jax.ShapeDtypeStruct((1, tok, half * width), BF16),
        in_specs=[pl.BlockSpec(memory_space=pl.ANY)] * 3 + [pl.BlockSpec(memory_space=pltpu.VMEM)] * 3,
        out_specs=pl.BlockSpec(memory_space=pltpu.VMEM),
        scratch_shapes=[
            pltpu.VMEM(up.shape, BF16),
            pltpu.VMEM(down.shape, BF16),
            pltpu.VMEM(spare.shape, BF16),
            pltpu.VMEM((n_chunk, n_tensor, M, width), BF16),
            pltpu.VMEM((LAG_B + 1, M, hidden), F32),
            pltpu.VMEM((LAG_B + 1, M, 128), F32),
            pltpu.VMEM((n_chunk, M, hidden + 128), BF16),
            pltpu.VMEM((n_chunk, M, hidden + 128), BF16),
            pltpu.VMEM((n_tensor, M, width), F32),
            pltpu.VMEM((n_chunk, n_tensor, M, width), BF16),
            pltpu.VMEM((n_chunk, n_tensor - 1, M, width), BF16),
            pltpu.VMEM((n_chunk, M, width), BF16),
            pltpu.VMEM((half, tok, width), BF16),
            dma((n_chunk,)),
            dma((n_chunk, 2)),
            dma((n_chunk,)),
            dma,
            dma((n_chunk,)),
            dma((n_chunk,)),
            dma((n_chunk,)),
            dma((n_live,)),
            dma((2, 2, n_tensor)),
        ],
        compiler_params=pltpu.CompilerParams(has_side_effects=True, vmem_limit_bytes=60 * 1024 * 1024),
    )(up, down, spare, lost, gain, entering)


def by_columns(n_tensor, backup_up, backup_down):
    rows, width = backup_up.shape[0], backup_up.shape[1] // n_tensor
    dma = pltpu.SemaphoreType.DMA
    return pl.pallas_call(
        functools.partial(exchange, n_tensor),
        out_shape=jax.ShapeDtypeStruct((2, width // BLOCK, BLOCK, BLOCK), BF16),
        in_specs=[pl.BlockSpec(memory_space=pltpu.VMEM)] * 2,
        out_specs=pl.BlockSpec(memory_space=pltpu.VMEM),
        scratch_shapes=[
            pltpu.VMEM((n_tensor, rows, width), BF16),
            pltpu.VMEM((n_tensor, rows, width), BF16),
            dma((n_tensor - 1, 2)),
            dma((n_tensor - 1, 2)),
            dma((2,)),
        ],
        compiler_params=pltpu.CompilerParams(has_side_effects=True),
    )(backup_up, backup_down)


def turned(n_tensor, down):
    rows, hidden = down.shape
    width = rows // n_tensor

    def turn(down_ref, out_ref):
        out_ref[0] = down_ref[...].astype(F32).T.astype(BF16)

    return pl.pallas_call(
        turn,
        grid=(n_tensor, hidden // BLOCK),
        out_shape=jax.ShapeDtypeStruct((n_tensor, hidden, width), BF16),
        in_specs=[pl.BlockSpec((width, BLOCK), lambda j, i: (j, i))],
        out_specs=pl.BlockSpec((1, BLOCK, width), lambda j, i: (j, i, 0)),
        cost_estimate=pl.CostEstimate(flops=0, bytes_accessed=16 * rows * hidden, transcendentals=0),
    )(down)


def cut_up(micro_batches, live_count, width):
    count, rows, share = micro_batches.shape

    def cut(live_ref, mb_ref, out_ref):
        factor = (pl.program_id(0) < live_ref[0]).astype(F32)
        for k in range(share // width):
            out_ref[0, k] = (mb_ref[0, :, k * width : (k + 1) * width].astype(F32) * factor).astype(BF16)

    return pl.pallas_call(
        cut,
        grid=(count,),
        out_shape=jax.ShapeDtypeStruct((count, share // width, rows, width), BF16),
        in_specs=[
            pl.BlockSpec(memory_space=pltpu.SMEM),
            pl.BlockSpec((1, rows, share), lambda b: (b, 0, 0)),
        ],
        out_specs=pl.BlockSpec((1, share // width, rows, width), lambda b: (b, 0, 0, 0)),
        cost_estimate=pl.CostEstimate(flops=0, bytes_accessed=16 * count * rows * share, transcendentals=0),
    )(live_count.reshape(1), micro_batches)


def body(
    mesh,
    section_up,
    section_down,
    backup_up,
    backup_down,
    norm_gain,
    micro_batches,
    failed_section,
    live_batches,
):
    n_tensor = lax.axis_size("tensor")
    pieces = by_columns(n_tensor, backup_up[0, 0, 0], backup_down[0, 0, 0])
    spare = lax.all_gather(pieces, "section", axis=0)
    rows = section_up.shape[1]
    is_failed = lax.axis_index("section") == failed_section[0] % lax.axis_size("section")
    lost = jnp.broadcast_to(is_failed.astype(BF16), (16, BLOCK))
    own_down = turned(n_tensor, section_down[0])
    batch_count = micro_batches.shape[0]
    live_count = batch_count // 2 + live_batches[0] % (batch_count - batch_count // 2 + 1)
    entering = cut_up(micro_batches, live_count, rows // n_tensor)
    fewest = batch_count // 2
    sizes = list(range(fewest, batch_count, STEP)) + [batch_count]
    return lax.switch(
        (live_count - fewest + STEP - 1) // STEP,
        [functools.partial(pipelined, mesh, n_live) for n_live in sizes],
        section_up[0],
        own_down,
        spare,
        lost,
        norm_gain,
        entering,
    )


def solution(mesh):
    placed = (
        P("section", "dp", "tensor"),
        P("section", "dp", "tensor"),
        P("dp", "section", "tensor", None, None),
        P("dp", "section", "tensor", None, None),
        P("section", None),
        P(None, "dp", "tensor"),
        P(),
        P(),
    )
    return jax.shard_map(
        functools.partial(body, mesh),
        mesh=mesh,
        in_specs=placed,
        out_specs=P("section", "dp", "tensor"),
        check_vma=False,
    )
```
